32 devices in a mesh: tok: 8 (over z, y), unit: 4 (over x, core).
Axes of the slice: x: 2, y: 2, z: 4, core: 2. Of those that a mesh axis runs over, the one named last changes fastest.
Arguments:
- act_a: bfloat16 [16384, 3072], P('tok', 'unit'), may hold values from -4000 to 4000
- act_b: bfloat16 [16384, 3072], P(('tok', 'unit')), may hold values from -4000 to 4000
Outputs:
- correlation: float32 [3072, 3072], P('tok', 'unit')
The draws below stay inside these ranges and needn't reach their ends.
All inputs are finite; a program needn't handle non-finite values.
Results may differ from the reference program's by a relative error of at most 0.0003.
Values may be sent and summed in bfloat16 or wider, within the bound.
A program may use at most 128 MiB of HBM per device.

```python
import math
import jax
import jax.numpy as jnp
from jax import lax

U = 3072
TOK_DEV = 2048
TOKENS = 16384
N_TOK = 8


def shared_parts(key):
    latent = jnp.clip(jax.random.normal(jax.random.fold_in(key, 101), (TOKENS, U), jnp.float32), -6.0, 6.0)
    position = jnp.arange(TOKENS, dtype=jnp.float32) / TOKENS
    growth = math.log(3.0)
    jitter = jax.random.uniform(jax.random.fold_in(key, 102), (TOKENS,), jnp.float32, -0.6, 0.6)
    token_scale = jnp.exp(growth * position + jitter)
    return (latent, token_scale)


def own_noise(key):
    return jnp.clip(jax.random.normal(key, (TOKENS, U), jnp.float32), -6.0, 6.0)


def draw_act_a(key, part):
    latent, token_scale = shared_parts(key)
    own_key = jax.random.fold_in(key, 201)
    unit_scale = jnp.exp(jax.random.uniform(jax.random.fold_in(own_key, 1), (U,), jnp.float32, 0.0, math.log(10.0)))
    offset = jnp.clip(jax.random.normal(jax.random.fold_in(own_key, 2), (U,), jnp.float32), -3.0, 3.0)
    noise = own_noise(jax.random.fold_in(own_key, 3))
    value = unit_scale[None, :] * token_scale[:, None] * (offset[None, :] + latent + 0.7 * noise)
    return value.astype(jnp.bfloat16)


def draw_act_b(key, part):
    latent, token_scale = shared_parts(key)
    own_key = jax.random.fold_in(key, 301)
    unit_scale = jnp.exp(jax.random.uniform(jax.random.fold_in(own_key, 1), (U,), jnp.float32, 0.0, math.log(10.0)))
    offset = jnp.clip(jax.random.normal(jax.random.fold_in(own_key, 2), (U,), jnp.float32), -3.0, 3.0)
    noise = own_noise(jax.random.fold_in(own_key, 3))
    order = jax.random.permutation(jax.random.fold_in(own_key, 4), U)
    weight = jax.random.uniform(jax.random.fold_in(own_key, 5), (U,), jnp.float32, -1.2, 1.2)
    moved = jnp.take(latent, order, axis=1)
    value = unit_scale[None, :] * token_scale[:, None] * (offset[None, :] + weight[None, :] * moved + 0.7 * noise)
    return value.astype(jnp.bfloat16)


def setup_inputs(seed: int = 0) -> dict:
    keys = jax.random.split(jax.random.key(seed), 3)
    act_a = draw_act_a(jax.random.fold_in(keys[2], 71), 0)
    act_b = draw_act_b(jax.random.fold_in(keys[2], 71), 0)
    return dict(act_a=act_a, act_b=act_b)


def reference(act_a, act_b):

    def step(carry, index):
        raw, first_total, first_square, second_total, second_square = carry
        start = (index * TOK_DEV).astype(jnp.int32)
        block_a = lax.dynamic_slice_in_dim(act_a, start, TOK_DEV, 0)
        block_b = lax.dynamic_slice_in_dim(act_b, start, TOK_DEV, 0)
        raw = raw + jnp.dot(block_b.T, block_a, preferred_element_type=jnp.float32)
        wide_a = block_a.astype(jnp.float32)
        wide_b = block_b.astype(jnp.float32)
        first_total = first_total + lax.optimization_barrier(jnp.sum(wide_a, axis=0))
        first_square = first_square + lax.optimization_barrier(jnp.sum(wide_a * wide_a, axis=0))
        second_total = second_total + lax.optimization_barrier(jnp.sum(wide_b, axis=0))
        second_square = second_square + lax.optimization_barrier(jnp.sum(wide_b * wide_b, axis=0))
        return ((raw, first_total, first_square, second_total, second_square), None)
    zeros_unit = jnp.zeros((U,), jnp.float32)
    start_carry = (jnp.zeros((U, U), jnp.float32), zeros_unit, zeros_unit, zeros_unit, zeros_unit)
    final, _ = lax.scan(step, start_carry, jnp.arange(N_TOK, dtype=jnp.int32))
    raw, first_total, first_square, second_total, second_square = final
    mean_a = first_total / TOKENS
    var_a = first_square / TOKENS - mean_a * mean_a
    mean_b = second_total / TOKENS
    var_b = second_square / TOKENS - mean_b * mean_b
    centered = raw / TOKENS - mean_b[:, None] * mean_a[None, :]
    return centered / (jnp.sqrt(var_b + 1e-05)[:, None] * jnp.sqrt(var_a + 1e-05)[None, :])
```

```python
import functools

import jax
import jax.numpy as jnp
from jax import lax
from jax.experimental import pallas as pl
from jax.experimental.pallas import tpu as pltpu
from jax.sharding import PartitionSpec as P

MESH = pl.DeviceIdType.MESH
LANES = 128
SPAN = 240.0
BASE = 120.0


def contract_tokens(left, right):
    return lax.dot_general(
        left, right, (((0,), (0,)), ((), ())), preferred_element_type=jnp.float32
    )


def plain(act_a, act_b):
    token_rows = act_a.shape[0]
    units = act_b.shape[1]
    groups = lax.axis_size("tok")
    band = units // groups
    total_tokens = token_rows * groups
    wide_a = act_a.astype(jnp.float32)
    first_total = jnp.sum(wide_a, axis=0)
    first_square = jnp.sum(wide_a * wide_a, axis=0)
    piece = lax.all_gather(act_b, "unit", axis=0, tiled=True)
    product = contract_tokens(piece, act_a)
    wide_piece = piece.astype(jnp.float32)
    second_total = jnp.sum(wide_piece, axis=0)
    second_square = jnp.sum(wide_piece * wide_piece, axis=0)
    shares = lax.psum_scatter(product, "tok", scatter_dimension=0, tiled=True)
    first_all, first_square_all, second_all, second_square_all = lax.psum(
        (first_total, first_square, second_total, second_square), "tok"
    )
    offset = lax.axis_index("tok") * band
    second_own = lax.dynamic_slice_in_dim(second_all, offset, band, 0)
    second_square_own = lax.dynamic_slice_in_dim(second_square_all, offset, band, 0)
    mean_a = first_all / total_tokens
    var_a = first_square_all / total_tokens - mean_a * mean_a
    mean_b = second_own / total_tokens
    var_b = second_square_own / total_tokens - mean_b * mean_b
    centered = shares / total_tokens - mean_b[:, None] * mean_a[None, :]
    return centered / (jnp.sqrt(var_b + 1e-05)[:, None] * jnp.sqrt(var_a + 1e-05)[None, :])


def step_order(groups):
    rings = groups // 2
    def far(o):
        d = o // 2
        return min(d, rings - d)
    return sorted(range(groups), key=lambda o: (-far(o), -(o % 2), o))


def column(row):
    return jnp.transpose(jnp.broadcast_to(row, (LANES, LANES)))


def spread(square, total, tokens):
    return jnp.maximum(square - total * total * (1.0 / tokens), square * 1e-5 + 1e-30)


def kernel(groups, order, a_hbm, b_hbm, out, a, gathered, codes, arrived, acc,
           sa_own, sa_all, sb_own, sb_all,
           a_sem, local_sem, px_send, px_recv, nx_send, nx_recv, fw_send, fw_recv,
           y_send, y_recv, sa_send, sa_recv, sb_send, sb_recv):
    t = lax.axis_index("tok")
    u = lax.axis_index("unit")
    rows, units = b_hbm.shape
    tokens, own = a.shape
    band = units // groups
    total_tokens = tokens * groups
    rings = groups // 2
    last = groups - 1
    partner = u + 1 - 2 * (u % 2)
    across = (u + 2) % 4

    def offset(s):
        o = jnp.int32(order[last])
        for i in range(last):
            o = jnp.where(s == i, order[i], o)
        return o

    def target(s):
        o = offset(s)
        return ((t // 2 + o // 2) % rings) * 2 + (t % 2 + o % 2) % 2

    def own_block(s):
        return b_hbm.at[:, pl.ds(pl.multiple_of(target(s) * band, LANES), band)]

    def slot(s, who):
        return gathered.at[s, pl.ds(pl.multiple_of(who * rows, rows), rows), :]

    def local_copy(s):
        return pltpu.make_async_copy(own_block(s), slot(s, u), local_sem.at[s])

    def remote(src, dst, send, recv, s, tt, uu):
        return pltpu.make_async_remote_copy(
            src_ref=src, dst_ref=dst, send_sem=send.at[s], recv_sem=recv.at[s],
            device_id=(tt, uu), device_id_type=MESH)

    def to_partner(s):
        return remote(own_block(s), slot(s, u), px_send, px_recv, s, t, partner)

    def to_across(s):
        return remote(own_block(s), slot(s, u), nx_send, nx_recv, s, t, across)

    def forward(s):
        return remote(slot(s, across), slot(s, across), fw_send, fw_recv, s, t, partner)

    def send_codes(s):
        return remote(codes.at[s], arrived.at[s], y_send, y_recv, s, target(s), u)

    def send_sa(s):
        return remote(sa_own, sa_all.at[s], sa_send, sa_recv, s, target(s), u)

    def send_sb(s):
        return remote(sb_own.at[s], sb_all.at[s], sb_send, sb_recv, s, target(s), u)

    a_copy = pltpu.make_async_copy(a_hbm, a, a_sem)
    a_copy.start()

    barrier = pltpu.get_barrier_semaphore()

    @pl.loop(0, last)
    def _(s):
        pl.semaphore_signal(barrier, inc=1, device_id=(target(s), u), device_id_type=MESH)

    pl.semaphore_signal(barrier, inc=1, device_id=(t, partner), device_id_type=MESH)
    pl.semaphore_signal(barrier, inc=1, device_id=(t, across), device_id_type=MESH)
    pl.semaphore_wait(barrier, groups + 1)

    @pl.loop(0, groups)
    def _(s):
        to_across(s).start()
        to_partner(s).start()
        local_copy(s).start()

    a_copy.wait()
    chunk = 128

    def sums(read, width):
        def body(i, carry):
            total, square = carry
            wide = read(pl.ds(pl.multiple_of(i * chunk, chunk), chunk)).astype(jnp.float32)
            wide = wide.reshape(chunk // 8, 8, width)
            return total + jnp.sum(wide, axis=0), square + jnp.sum(wide * wide, axis=0)
        zero = jnp.zeros((8, width), jnp.float32)
        total, square = lax.fori_loop(0, tokens // chunk, body, (zero, zero))
        return (jnp.sum(total, axis=0, keepdims=True), jnp.sum(square, axis=0, keepdims=True))

    total, square = sums(lambda r: a[r, :], own)
    sa_own[0:1, :] = total
    sa_own[1:2, :] = square
    sa_own[2:8, :] = jnp.zeros((6, own), jnp.float32)
    sa_all[last] = jnp.zeros((8, own), jnp.float32)
    sa_all[last, 0:1, :] = total
    sa_all[last, 1:2, :] = square

    @pl.loop(0, last)
    def _(s):
        send_sa(s).start()

    def product(s, keep):
        @pl.loop(0, band // LANES)
        def _(i):
            lanes = pl.ds(pl.multiple_of(i * LANES, LANES), LANES)
            tb, qb = sums(lambda r: gathered[s, r, lanes], LANES)
            if keep:
                sb_all[last, 0:1, lanes] = tb
                sb_all[last, 1:2, lanes] = qb
            else:
                sb_own[s, 0:1, lanes] = tb
                sb_own[s, 1:2, lanes] = qb
            raw = contract_tokens(gathered[s, :, lanes], a[...])
            tb_col = column(tb) * (1.0 / tokens)
            scale_col = column(lax.rsqrt(spread(qb, tb, tokens)))
            for c in range(own // LANES):
                cols = slice(c * LANES, (c + 1) * LANES)
                part = raw[:, cols]
                if keep:
                    acc[lanes, cols] = part
                else:
                    ta = sa_own[0:1, cols]
                    scale = lax.rsqrt(spread(sa_own[1:2, cols], ta, tokens))
                    q = (part - tb_col * ta) * (scale_col * scale)
                    size = jnp.exp2(jnp.minimum(jnp.abs(q), 1.04) * SPAN - BASE)
                    codes[s, lanes, cols] = jnp.where(q < 0, -size, size).astype(jnp.bfloat16)

    def gather_step(s):
        local_copy(s).wait()
        to_across(s).wait_recv()
        forward(s).start()
        to_partner(s).wait_recv()
        forward(s).wait_recv()

    sb_all[last] = jnp.zeros((8, band), jnp.float32)

    @pl.loop(0, last)
    def _(s):
        sb_own[s] = jnp.zeros((8, band), jnp.float32)
        gather_step(s)
        product(s, False)
        send_codes(s).start()
        send_sb(s).start()

    gather_step(last)
    product(last, True)

    @pl.loop(0, last)
    def _(s):
        send_sa(s).wait_recv()
        send_sb(s).wait_recv()
        send_codes(s).wait_recv()

        @pl.loop(0, band // LANES)
        def _(i):
            lanes = pl.ds(pl.multiple_of(i * LANES, LANES), LANES)
            tb = sb_all[s, 0:1, lanes]
            qb = sb_all[s, 1:2, lanes]
            tb_col = column(tb) * (1.0 / tokens)
            norm_col = column(jnp.sqrt(spread(qb, tb, tokens))) * (1.0 / SPAN)
            for c in range(own // LANES):
                cols = slice(c * LANES, (c + 1) * LANES)
                ta = sa_all[s, 0:1, cols]
                norm = jnp.sqrt(spread(sa_all[s, 1:2, cols], ta, tokens))
                y = arrived[s, lanes, cols].astype(jnp.float32)
                size = jnp.log2(jnp.abs(y)) + BASE
                q = jnp.where(y < 0, -size, size)
                acc[lanes, cols] = acc[lanes, cols] + (q * (norm_col * norm) + tb_col * ta)

    whole_b = jnp.sum(sb_all[...], axis=0)
    whole_a = jnp.sum(sa_all[...], axis=0)
    mean_a = whole_a[0:1, :] * (1.0 / total_tokens)
    var_a = whole_a[1:2, :] * (1.0 / total_tokens) - mean_a * mean_a
    inv_a = 1.0 / jnp.sqrt(var_a + 1e-05)
    mean_b = whole_b[0:1, :] * (1.0 / total_tokens)
    var_b = whole_b[1:2, :] * (1.0 / total_tokens) - mean_b * mean_b
    inv_b = 1.0 / jnp.sqrt(var_b + 1e-05)
    for i in range(band // LANES):
        lanes = slice(i * LANES, (i + 1) * LANES)
        mean_col = column(mean_b[:, lanes])
        inv_col = column(inv_b[:, lanes])
        for c in range(own // LANES):
            cols = slice(c * LANES, (c + 1) * LANES)
            centered = acc[lanes, cols] * (1.0 / total_tokens) - mean_col * mean_a[:, cols]
            out[lanes, cols] = centered * (inv_col * inv_a[:, cols])

    @pl.loop(0, last)
    def _(s):
        send_sa(s).wait_send()
        send_sb(s).wait_send()
        send_codes(s).wait_send()

    @pl.loop(0, groups)
    def _(s):
        to_across(s).wait_send()
        to_partner(s).wait_send()
        forward(s).wait_send()


def fused(groups, act_a, act_b):
    tokens, own = act_a.shape
    rows, units = act_b.shape
    band = units // groups
    last = groups - 1
    dma = lambda n: pltpu.SemaphoreType.DMA((n,))
    return pl.pallas_call(
        functools.partial(kernel, groups, step_order(groups)),
        out_shape=jax.ShapeDtypeStruct((band, own), jnp.float32),
        in_specs=[pl.BlockSpec(memory_space=pltpu.HBM)] * 2,
        out_specs=pl.BlockSpec(memory_space=pltpu.VMEM),
        scratch_shapes=[
            pltpu.VMEM((tokens, own), jnp.bfloat16),
            pltpu.VMEM((groups, tokens, band), jnp.bfloat16),
            pltpu.VMEM((last, band, own), jnp.bfloat16),
            pltpu.VMEM((last, band, own), jnp.bfloat16),
            pltpu.VMEM((band, own), jnp.float32),
            pltpu.VMEM((8, own), jnp.float32),
            pltpu.VMEM((groups, 8, own), jnp.float32),
            pltpu.VMEM((last, 8, band), jnp.float32),
            pltpu.VMEM((groups, 8, band), jnp.float32),
            pltpu.SemaphoreType.DMA,
            dma(groups),
            dma(groups), dma(groups),
            dma(groups), dma(groups),
            dma(groups), dma(groups),
            dma(last), dma(last),
            dma(last), dma(last),
            dma(last), dma(last),
        ],
        compiler_params=pltpu.CompilerParams(
            collective_id=0, has_side_effects=True, vmem_limit_bytes=60000 * 1024
        ),
        name="gather_correlate",
    )(act_a, act_b)


def solution(mesh):
    groups, split = mesh.shape["tok"], mesh.shape["unit"]

    def per_device(act_a, act_b):
        band = act_b.shape[1] // groups
        whole = act_a.shape[0] % 128 == 0 and act_a.shape[1] % LANES == 0
        if split == 4 and groups % 2 == 0 and band % LANES == 0 and whole:
            return fused(groups, act_a, act_b)
        return plain(act_a, act_b)

    placed = (P("tok", "unit"), P(("tok", "unit"), None))
    return jax.shard_map(
        per_device, mesh=mesh, in_specs=placed, out_specs=P("tok", "unit"), check_vma=False
    )
```

```python
import functools

import jax
import jax.numpy as jnp
from jax import lax
from jax.experimental import pallas as pl
from jax.experimental.pallas import tpu as pltpu
from jax.sharding import PartitionSpec as P

MESH = pl.DeviceIdType.MESH
LANES = 128
SPAN = 240.0
BASE = 120.0


def contract_tokens(left, right):
    return lax.dot_general(
        left, right, (((0,), (0,)), ((), ())), preferred_element_type=jnp.float32
    )


def plain(act_a, act_b):
    token_rows = act_a.shape[0]
    units = act_b.shape[1]
    groups = lax.axis_size("tok")
    band = units // groups
    total_tokens = token_rows * groups
    wide_a = act_a.astype(jnp.float32)
    first_total = jnp.sum(wide_a, axis=0)
    first_square = jnp.sum(wide_a * wide_a, axis=0)
    piece = lax.all_gather(act_b, "unit", axis=0, tiled=True)
    product = contract_tokens(piece, act_a)
    wide_piece = piece.astype(jnp.float32)
    second_total = jnp.sum(wide_piece, axis=0)
    second_square = jnp.sum(wide_piece * wide_piece, axis=0)
    shares = lax.psum_scatter(product, "tok", scatter_dimension=0, tiled=True)
    first_all, first_square_all, second_all, second_square_all = lax.psum(
        (first_total, first_square, second_total, second_square), "tok"
    )
    offset = lax.axis_index("tok") * band
    second_own = lax.dynamic_slice_in_dim(second_all, offset, band, 0)
    second_square_own = lax.dynamic_slice_in_dim(second_square_all, offset, band, 0)
    mean_a = first_all / total_tokens
    var_a = first_square_all / total_tokens - mean_a * mean_a
    mean_b = second_own / total_tokens
    var_b = second_square_own / total_tokens - mean_b * mean_b
    centered = shares / total_tokens - mean_b[:, None] * mean_a[None, :]
    return centered / (jnp.sqrt(var_b + 1e-05)[:, None] * jnp.sqrt(var_a + 1e-05)[None, :])


def pair_order(rings):
    return sorted(range(rings), key=lambda d: (-min(d, rings - d), d))


def column(row):
    return jnp.transpose(jnp.broadcast_to(row, (LANES, LANES)))


def spread(square, total, tokens):
    return jnp.maximum(square - total * total * (1.0 / tokens), square * 1e-5 + 1e-30)


def encode(q):
    size = jnp.exp2(jnp.minimum(jnp.abs(q), 1.04) * SPAN - BASE)
    return jnp.where(q < 0, -size, size).astype(jnp.bfloat16)


def decode(code):
    y = code.astype(jnp.float32)
    size = jnp.log2(jnp.abs(y)) + BASE
    return jnp.where(y < 0, -size, size)


def kernel(groups, order, a_hbm, b_hbm, out, a, gathered, cross_out, cross_in, far_out, far_in,
           held, sa_own, sa_near, sa_pair, sa_all, sb_cross, sb_near, sb_keep, sb_pair,
           a_sem, local_sem, px_send, px_recv, nx_send, nx_recv, fw_send, fw_recv,
           c_send, c_recv, f_send, f_recv, cb_send, cb_recv, fb_send, fb_recv,
           ca_send, ca_recv, fa_send, fa_recv):
    t = lax.axis_index("tok")
    u = lax.axis_index("unit")
    rows, units = b_hbm.shape
    tokens, own = a.shape
    band = units // groups
    total_tokens = tokens * groups
    rings = groups // 2
    last = rings - 1
    partner = u + 1 - 2 * (u % 2)
    across = (u + 2) % 4
    near = t + 1 - 2 * (t % 2)

    def shift(p):
        d = jnp.int32(order[last])
        for i in range(last):
            d = jnp.where(p == i, order[i], d)
        return d

    def peer(p):
        return ((t // 2 + shift(p)) % rings) * 2 + t % 2

    def target(s):
        return ((t // 2 + shift(s // 2)) % rings) * 2 + (t + 1 + s) % 2

    def own_block(s):
        return b_hbm.at[:, pl.ds(pl.multiple_of(target(s) * band, LANES), band)]

    def slot(s, who):
        return gathered.at[s, pl.ds(pl.multiple_of(who * rows, rows), rows), :]

    def local_copy(s):
        return pltpu.make_async_copy(own_block(s), slot(s, u), local_sem.at[s])

    def remote(src, dst, send, recv, s, tt, uu):
        return pltpu.make_async_remote_copy(
            src_ref=src, dst_ref=dst, send_sem=send.at[s], recv_sem=recv.at[s],
            device_id=(tt, uu), device_id_type=MESH)

    def to_partner(s):
        return remote(own_block(s), slot(s, u), px_send, px_recv, s, t, partner)

    def to_across(s):
        return remote(own_block(s), slot(s, u), nx_send, nx_recv, s, t, across)

    def forward(s):
        return remote(slot(s, across), slot(s, across), fw_send, fw_recv, s, t, partner)

    def send_cross(p):
        return remote(cross_out.at[p], cross_in.at[p], c_send, c_recv, p, near, u)

    def send_cross_sums(p):
        return remote(sb_cross.at[p], sb_near.at[p], cb_send, cb_recv, p, near, u)

    def send_far(p):
        return remote(far_out.at[p], far_in.at[p], f_send, f_recv, p, peer(p), u)

    def send_far_sums(p):
        return remote(sb_keep.at[p], sb_pair.at[p], fb_send, fb_recv, p, peer(p), u)

    send_near_a = remote(sa_own, sa_near, ca_send, ca_recv, 0, near, u)

    def send_far_a(p):
        return remote(sa_pair, sa_all.at[p], fa_send, fa_recv, p, peer(p), u)

    a_copy = pltpu.make_async_copy(a_hbm, a, a_sem)
    a_copy.start()

    barrier = pltpu.get_barrier_semaphore()

    @pl.loop(0, last)
    def _(p):
        pl.semaphore_signal(barrier, inc=1, device_id=(peer(p), u), device_id_type=MESH)

    pl.semaphore_signal(barrier, inc=1, device_id=(near, u), device_id_type=MESH)
    pl.semaphore_signal(barrier, inc=1, device_id=(t, partner), device_id_type=MESH)
    pl.semaphore_signal(barrier, inc=1, device_id=(t, across), device_id_type=MESH)
    pl.semaphore_wait(barrier, rings + 2)

    @pl.loop(0, groups)
    def _(s):
        to_across(s).start()
        to_partner(s).start()
        local_copy(s).start()

    a_copy.wait()
    chunk = 128

    def sums(read, width):
        def body(i, carry):
            total, square = carry
            wide = read(pl.ds(pl.multiple_of(i * chunk, chunk), chunk)).astype(jnp.float32)
            wide = wide.reshape(chunk // 8, 8, width)
            return total + jnp.sum(wide, axis=0), square + jnp.sum(wide * wide, axis=0)
        zero = jnp.zeros((8, width), jnp.float32)
        total, square = lax.fori_loop(0, tokens // chunk, body, (zero, zero))
        return (jnp.sum(total, axis=0, keepdims=True), jnp.sum(square, axis=0, keepdims=True))

    total, square = sums(lambda r: a[r, :], own)
    sa_own[...] = jnp.zeros((8, own), jnp.float32)
    sa_own[0:1, :] = total
    sa_own[1:2, :] = square
    send_near_a.start()

    def product(p, s, keep):
        sums_ref = sb_keep if keep else sb_cross
        sums_ref[p] = jnp.zeros((8, band), jnp.float32)

        @pl.loop(0, band // LANES)
        def _(i):
            lanes = pl.ds(pl.multiple_of(i * LANES, LANES), LANES)
            tb, qb = sums(lambda r: gathered[s, r, lanes], LANES)
            sums_ref[p, 0:1, lanes] = tb
            sums_ref[p, 1:2, lanes] = qb
            raw = contract_tokens(gathered[s, :, lanes], a[...])
            if keep:
                held[p, lanes, :] = raw
                return
            tb_col = column(tb) * (1.0 / tokens)
            scale_col = column(lax.rsqrt(spread(qb, tb, tokens)))
            for c in range(own // LANES):
                cols = slice(c * LANES, (c + 1) * LANES)
                ta = sa_own[0:1, cols]
                scale = lax.rsqrt(spread(sa_own[1:2, cols], ta, tokens))
                q = (raw[:, cols] - tb_col * ta) * (scale_col * scale)
                cross_out[p, lanes, cols] = encode(q)

    def gather_step(s):
        local_copy(s).wait()
        to_across(s).wait_recv()
        forward(s).start()
        to_partner(s).wait_recv()
        forward(s).wait_recv()

    def combine(p, send):
        send_cross_sums(p).wait_recv()
        send_cross(p).wait_recv()

        @pl.loop(0, band // LANES)
        def _(i):
            lanes = pl.ds(pl.multiple_of(i * LANES, LANES), LANES)
            tb = sb_near[p, 0:1, lanes]
            qb = sb_near[p, 1:2, lanes]
            tb_col = column(tb) * (1.0 / tokens)
            norm_col = column(jnp.sqrt(spread(qb, tb, tokens))) * (1.0 / SPAN)
            tb2 = tb + sb_keep[p, 0:1, lanes]
            qb2 = qb + sb_keep[p, 1:2, lanes]
            sb_keep[p, 0:1, lanes] = tb2
            sb_keep[p, 1:2, lanes] = qb2
            tb2_col = column(tb2) * (0.5 / tokens)
            scale_col = column(lax.rsqrt(spread(qb2, tb2, 2 * tokens)))
            for c in range(own // LANES):
                cols = slice(c * LANES, (c + 1) * LANES)
                ta = sa_near[0:1, cols]
                norm = jnp.sqrt(spread(sa_near[1:2, cols], ta, tokens))
                raw = held[p, lanes, cols] + (
                    decode(cross_in[p, lanes, cols]) * (norm_col * norm) + tb_col * ta)
                if send:
                    ta2 = sa_pair[0:1, cols]
                    scale = lax.rsqrt(spread(sa_pair[1:2, cols], ta2, 2 * tokens))
                    q = (raw - tb2_col * ta2) * (scale_col * scale)
                    far_out[p, lanes, cols] = encode(q)
                else:
                    held[p, lanes, cols] = raw

        if send:
            send_far(p).start()
            send_far_sums(p).start()

    def arrive(p):
        send_far_a(p).wait_recv()
        send_far_sums(p).wait_recv()
        send_far(p).wait_recv()

        @pl.loop(0, band // LANES)
        def _(i):
            lanes = pl.ds(pl.multiple_of(i * LANES, LANES), LANES)
            tb = sb_pair[p, 0:1, lanes]
            qb = sb_pair[p, 1:2, lanes]
            tb_col = column(tb) * (0.5 / tokens)
            norm_col = column(jnp.sqrt(spread(qb, tb, 2 * tokens))) * (1.0 / SPAN)
            for c in range(own // LANES):
                cols = slice(c * LANES, (c + 1) * LANES)
                ta = sa_all[p, 0:1, cols]
                norm = jnp.sqrt(spread(sa_all[p, 1:2, cols], ta, 2 * tokens))
                held[last, lanes, cols] = held[last, lanes, cols] + (
                    decode(far_in[p, lanes, cols]) * (norm_col * norm) + tb_col * ta)

    send_near_a.wait_recv()
    sa_pair[...] = sa_own[...] + sa_near[...]

    @pl.loop(0, last)
    def _(p):
        send_far_a(p).start()

    @pl.loop(0, rings)
    def _(p):
        gather_step(2 * p)
        product(p, 2 * p, False)
        send_cross(p).start()
        send_cross_sums(p).start()

        @pl.when(p >= 1)
        def _():
            combine(p - 1, True)

        gather_step(2 * p + 1)
        product(p, 2 * p + 1, True)

    @pl.loop(0, last - 1)
    def _(p):
        arrive(p)

    combine(last, False)
    arrive(last - 1)

    whole_b = jnp.sum(sb_pair[...], axis=0) + sb_keep[last]
    whole_a = jnp.sum(sa_all[...], axis=0) + sa_pair[...]
    mean_a = whole_a[0:1, :] * (1.0 / total_tokens)
    var_a = whole_a[1:2, :] * (1.0 / total_tokens) - mean_a * mean_a
    inv_a = 1.0 / jnp.sqrt(var_a + 1e-05)
    mean_b = whole_b[0:1, :] * (1.0 / total_tokens)
    var_b = whole_b[1:2, :] * (1.0 / total_tokens) - mean_b * mean_b
    inv_b = 1.0 / jnp.sqrt(var_b + 1e-05)
    for i in range(band // LANES):
        lanes = slice(i * LANES, (i + 1) * LANES)
        mean_col = column(mean_b[:, lanes])
        inv_col = column(inv_b[:, lanes])
        for c in range(own // LANES):
            cols = slice(c * LANES, (c + 1) * LANES)
            centered = held[last, lanes, cols] * (1.0 / total_tokens) - mean_col * mean_a[:, cols]
            out[lanes, cols] = centered * (inv_col * inv_a[:, cols])

    send_near_a.wait_send()

    @pl.loop(0, last)
    def _(p):
        send_far_a(p).wait_send()
        send_far_sums(p).wait_send()
        send_far(p).wait_send()

    @pl.loop(0, rings)
    def _(p):
        send_cross(p).wait_send()
        send_cross_sums(p).wait_send()

    @pl.loop(0, groups)
    def _(s):
        to_across(s).wait_send()
        to_partner(s).wait_send()
        forward(s).wait_send()


def fused(groups, act_a, act_b):
    tokens, own = act_a.shape
    rows, units = act_b.shape
    band = units // groups
    rings = groups // 2
    last = rings - 1
    dma = lambda n: pltpu.SemaphoreType.DMA((n,))
    return pl.pallas_call(
        functools.partial(kernel, groups, pair_order(rings)),
        out_shape=jax.ShapeDtypeStruct((band, own), jnp.float32),
        in_specs=[pl.BlockSpec(memory_space=pltpu.HBM)] * 2,
        out_specs=pl.BlockSpec(memory_space=pltpu.VMEM),
        scratch_shapes=[
            pltpu.VMEM((tokens, own), jnp.bfloat16),
            pltpu.VMEM((groups, tokens, band), jnp.bfloat16),
            pltpu.VMEM((rings, band, own), jnp.bfloat16),
            pltpu.VMEM((rings, band, own), jnp.bfloat16),
            pltpu.VMEM((last, band, own), jnp.bfloat16),
            pltpu.VMEM((last, band, own), jnp.bfloat16),
            pltpu.VMEM((rings, band, own), jnp.float32),
            pltpu.VMEM((8, own), jnp.float32),
            pltpu.VMEM((8, own), jnp.float32),
            pltpu.VMEM((8, own), jnp.float32),
            pltpu.VMEM((last, 8, own), jnp.float32),
            pltpu.VMEM((rings, 8, band), jnp.float32),
            pltpu.VMEM((rings, 8, band), jnp.float32),
            pltpu.VMEM((rings, 8, band), jnp.float32),
            pltpu.VMEM((last, 8, band), jnp.float32),
            pltpu.SemaphoreType.DMA,
            dma(groups),
            dma(groups), dma(groups),
            dma(groups), dma(groups),
            dma(groups), dma(groups),
            dma(rings), dma(rings),
            dma(last), dma(last),
            dma(rings), dma(rings),
            dma(last), dma(last),
            dma(1), dma(1),
            dma(last), dma(last),
        ],
        compiler_params=pltpu.CompilerParams(
            collective_id=0, has_side_effects=True, vmem_limit_bytes=60000 * 1024
        ),
        name="gather_correlate",
    )(act_a, act_b)


def solution(mesh):
    groups, split = mesh.shape["tok"], mesh.shape["unit"]

    def per_device(act_a, act_b):
        band = act_b.shape[1] // groups
        whole = act_a.shape[0] % 128 == 0 and act_a.shape[1] % LANES == 0
        if split == 4 and groups % 2 == 0 and groups > 4 and band % LANES == 0 and whole:
            return fused(groups, act_a, act_b)
        return plain(act_a, act_b)

    placed = (P("tok", "unit"), P(("tok", "unit"), None))
    return jax.shard_map(
        per_device, mesh=mesh, in_specs=placed, out_specs=P("tok", "unit"), check_vma=False
    )
```

```python
import functools

import jax
import jax.numpy as jnp
from jax import lax
from jax.experimental import pallas as pl
from jax.experimental.pallas import tpu as pltpu
from jax.sharding import PartitionSpec as P

MESH = pl.DeviceIdType.MESH
LANES = 128
SPAN = 240.0
BASE = 120.0


def contract_tokens(left, right):
    return lax.dot_general(
        left, right, (((0,), (0,)), ((), ())), preferred_element_type=jnp.float32
    )


def plain(act_a, act_b):
    token_rows = act_a.shape[0]
    units = act_b.shape[1]
    groups = lax.axis_size("tok")
    band = units // groups
    total_tokens = token_rows * groups
    wide_a = act_a.astype(jnp.float32)
    first_total = jnp.sum(wide_a, axis=0)
    first_square = jnp.sum(wide_a * wide_a, axis=0)
    piece = lax.all_gather(act_b, "unit", axis=0, tiled=True)
    product = contract_tokens(piece, act_a)
    wide_piece = piece.astype(jnp.float32)
    second_total = jnp.sum(wide_piece, axis=0)
    second_square = jnp.sum(wide_piece * wide_piece, axis=0)
    shares = lax.psum_scatter(product, "tok", scatter_dimension=0, tiled=True)
    first_all, first_square_all, second_all, second_square_all = lax.psum(
        (first_total, first_square, second_total, second_square), "tok"
    )
    offset = lax.axis_index("tok") * band
    second_own = lax.dynamic_slice_in_dim(second_all, offset, band, 0)
    second_square_own = lax.dynamic_slice_in_dim(second_square_all, offset, band, 0)
    mean_a = first_all / total_tokens
    var_a = first_square_all / total_tokens - mean_a * mean_a
    mean_b = second_own / total_tokens
    var_b = second_square_own / total_tokens - mean_b * mean_b
    centered = shares / total_tokens - mean_b[:, None] * mean_a[None, :]
    return centered / (jnp.sqrt(var_b + 1e-05)[:, None] * jnp.sqrt(var_a + 1e-05)[None, :])


def pair_order(rings):
    return sorted(range(rings), key=lambda d: (-min(d, rings - d), d))


def column(row):
    return jnp.transpose(jnp.broadcast_to(row, (LANES, LANES)))


def spread(square, total, tokens):
    return jnp.maximum(square - total * total * (1.0 / tokens), square * 1e-5 + 1e-30)


def encode(q):
    size = jnp.exp2(jnp.minimum(jnp.abs(q), 1.04) * SPAN - BASE)
    return jnp.where(q < 0, -size, size).astype(jnp.bfloat16)


def decode(code):
    y = code.astype(jnp.float32)
    size = jnp.log2(jnp.abs(y)) + BASE
    return jnp.where(y < 0, -size, size)


def kernel(groups, order, a_hbm, b_hbm, out, a, gathered, cross_out, cross_in, far_out, far_in,
           held, sa_own, sa_near, sa_pair, sa_all, sb_cross, sb_near, sb_keep, sb_pair,
           a_sem, local_sem, px_send, px_recv, nx_send, nx_recv, fw_send, fw_recv,
           c_send, c_recv, f_send, f_recv, cb_send, cb_recv, fb_send, fb_recv,
           ca_send, ca_recv, fa_send, fa_recv):
    t = lax.axis_index("tok")
    u = lax.axis_index("unit")
    rows, units = b_hbm.shape
    tokens, own = a.shape
    band = units // groups
    total_tokens = tokens * groups
    rings = groups // 2
    last = rings - 1
    partner = u + 1 - 2 * (u % 2)
    across = (u + 2) % 4
    near = t + 1 - 2 * (t % 2)

    def shift(p):
        d = jnp.int32(order[last])
        for i in range(last):
            d = jnp.where(p == i, order[i], d)
        return d

    def peer(p):
        return ((t // 2 + shift(p)) % rings) * 2 + t % 2

    def target(s):
        return ((t // 2 + shift(s // 2)) % rings) * 2 + (t + 1 + s) % 2

    def own_block(s):
        return b_hbm.at[:, pl.ds(pl.multiple_of(target(s) * band, LANES), band)]

    def slot(s, who):
        return gathered.at[s, pl.ds(pl.multiple_of(who * rows, rows), rows), :]

    def local_copy(s):
        return pltpu.make_async_copy(own_block(s), slot(s, u), local_sem.at[s])

    def remote(src, dst, send, recv, s, tt, uu):
        return pltpu.make_async_remote_copy(
            src_ref=src, dst_ref=dst, send_sem=send.at[s], recv_sem=recv.at[s],
            device_id=(tt, uu), device_id_type=MESH)

    def to_partner(s):
        return remote(own_block(s), slot(s, u), px_send, px_recv, s, t, partner)

    def to_across(s):
        return remote(own_block(s), slot(s, u), nx_send, nx_recv, s, t, across)

    def forward(s):
        return remote(slot(s, across), slot(s, across), fw_send, fw_recv, s, t, partner)

    def send_cross(p):
        return remote(cross_out.at[p], cross_in.at[p], c_send, c_recv, p, near, u)

    def send_cross_sums(p):
        return remote(sb_cross.at[p], sb_near.at[p], cb_send, cb_recv, p, near, u)

    def send_far(p):
        return remote(far_out.at[p], far_in.at[p], f_send, f_recv, p, peer(p), u)

    def send_far_sums(p):
        return remote(sb_keep.at[p], sb_pair.at[p], fb_send, fb_recv, p, peer(p), u)

    send_near_a = remote(sa_own, sa_near, ca_send, ca_recv, 0, near, u)

    def send_far_a(p):
        return remote(sa_pair, sa_all.at[p], fa_send, fa_recv, p, peer(p), u)

    a_copy = pltpu.make_async_copy(a_hbm, a, a_sem)
    a_copy.start()

    barrier = pltpu.get_barrier_semaphore()

    @pl.loop(0, last)
    def _(p):
        pl.semaphore_signal(barrier, inc=1, device_id=(peer(p), u), device_id_type=MESH)

    pl.semaphore_signal(barrier, inc=1, device_id=(near, u), device_id_type=MESH)
    pl.semaphore_signal(barrier, inc=1, device_id=(t, partner), device_id_type=MESH)
    pl.semaphore_signal(barrier, inc=1, device_id=(t, across), device_id_type=MESH)
    pl.semaphore_wait(barrier, rings + 2)

    def begin(s):
        to_across(s).start()
        to_partner(s).start()
        local_copy(s).start()

    begin(0)

    @pl.loop(1, last)
    def _(p):
        begin(2 * p)
        begin(2 * p - 1)

    begin(2 * last - 1)
    begin(2 * last)
    begin(2 * last + 1)

    a_copy.wait()
    chunk = 128

    def sums(read, width):
        def body(i, carry):
            total, square = carry
            wide = read(pl.ds(pl.multiple_of(i * chunk, chunk), chunk)).astype(jnp.float32)
            wide = wide.reshape(chunk // 8, 8, width)
            return total + jnp.sum(wide, axis=0), square + jnp.sum(wide * wide, axis=0)
        zero = jnp.zeros((8, width), jnp.float32)
        total, square = lax.fori_loop(0, tokens // chunk, body, (zero, zero))
        return (jnp.sum(total, axis=0, keepdims=True), jnp.sum(square, axis=0, keepdims=True))

    total, square = sums(lambda r: a[r, :], own)
    sa_own[...] = jnp.zeros((8, own), jnp.float32)
    sa_own[0:1, :] = total
    sa_own[1:2, :] = square
    send_near_a.start()

    def product(p, s, keep):
        sums_ref = sb_keep if keep else sb_cross
        sums_ref[p] = jnp.zeros((8, band), jnp.float32)

        @pl.loop(0, band // LANES)
        def _(i):
            lanes = pl.ds(pl.multiple_of(i * LANES, LANES), LANES)
            tb, qb = sums(lambda r: gathered[s, r, lanes], LANES)
            sums_ref[p, 0:1, lanes] = tb
            sums_ref[p, 1:2, lanes] = qb
            raw = contract_tokens(gathered[s, :, lanes], a[...])
            if keep:
                held[p, lanes, :] = raw
                return
            tb_col = column(tb) * (1.0 / tokens)
            scale_col = column(lax.rsqrt(spread(qb, tb, tokens)))
            for c in range(own // LANES):
                cols = slice(c * LANES, (c + 1) * LANES)
                ta = sa_own[0:1, cols]
                scale = lax.rsqrt(spread(sa_own[1:2, cols], ta, tokens))
                q = (raw[:, cols] - tb_col * ta) * (scale_col * scale)
                cross_out[p, lanes, cols] = encode(q)

    def gather_step(s):
        local_copy(s).wait()
        to_across(s).wait_recv()
        forward(s).start()
        to_partner(s).wait_recv()
        forward(s).wait_recv()

    def combine(p, send):
        send_cross_sums(p).wait_recv()
        send_cross(p).wait_recv()

        @pl.loop(0, band // LANES)
        def _(i):
            lanes = pl.ds(pl.multiple_of(i * LANES, LANES), LANES)
            tb = sb_near[p, 0:1, lanes]
            qb = sb_near[p, 1:2, lanes]
            tb_col = column(tb) * (1.0 / tokens)
            norm_col = column(jnp.sqrt(spread(qb, tb, tokens))) * (1.0 / SPAN)
            tb2 = tb + sb_keep[p, 0:1, lanes]
            qb2 = qb + sb_keep[p, 1:2, lanes]
            sb_keep[p, 0:1, lanes] = tb2
            sb_keep[p, 1:2, lanes] = qb2
            tb2_col = column(tb2) * (0.5 / tokens)
            scale_col = column(lax.rsqrt(spread(qb2, tb2, 2 * tokens)))
            for c in range(own // LANES):
                cols = slice(c * LANES, (c + 1) * LANES)
                ta = sa_near[0:1, cols]
                norm = jnp.sqrt(spread(sa_near[1:2, cols], ta, tokens))
                raw = held[p, lanes, cols] + (
                    decode(cross_in[p, lanes, cols]) * (norm_col * norm) + tb_col * ta)
                if send:
                    ta2 = sa_pair[0:1, cols]
                    scale = lax.rsqrt(spread(sa_pair[1:2, cols], ta2, 2 * tokens))
                    q = (raw - tb2_col * ta2) * (scale_col * scale)
                    far_out[p, lanes, cols] = encode(q)
                else:
                    held[p, lanes, cols] = raw

        if send:
            send_far(p).start()
            send_far_sums(p).start()

    def arrive(p):
        send_far_a(p).wait_recv()
        send_far_sums(p).wait_recv()
        send_far(p).wait_recv()

        @pl.loop(0, band // LANES)
        def _(i):
            lanes = pl.ds(pl.multiple_of(i * LANES, LANES), LANES)
            tb = sb_pair[p, 0:1, lanes]
            qb = sb_pair[p, 1:2, lanes]
            tb_col = column(tb) * (0.5 / tokens)
            norm_col = column(jnp.sqrt(spread(qb, tb, 2 * tokens))) * (1.0 / SPAN)
            for c in range(own // LANES):
                cols = slice(c * LANES, (c + 1) * LANES)
                ta = sa_all[p, 0:1, cols]
                norm = jnp.sqrt(spread(sa_all[p, 1:2, cols], ta, 2 * tokens))
                held[last, lanes, cols] = held[last, lanes, cols] + (
                    decode(far_in[p, lanes, cols]) * (norm_col * norm) + tb_col * ta)

    send_near_a.wait_recv()
    sa_pair[...] = sa_own[...] + sa_near[...]

    @pl.loop(0, last)
    def _(p):
        send_far_a(p).start()

    def cross(p):
        gather_step(2 * p)
        product(p, 2 * p, False)
        send_cross(p).start()
        send_cross_sums(p).start()

    def keep(p):
        gather_step(2 * p + 1)
        product(p, 2 * p + 1, True)

    @pl.loop(0, rings)
    def _(p):
        @pl.when(p < last)
        def _():
            cross(p)

        @pl.when(p >= 1)
        def _():
            keep(p - 1)
            combine(p - 1, True)

    cross(last)
    keep(last)

    @pl.loop(0, last - 1)
    def _(p):
        arrive(p)

    combine(last, False)
    arrive(last - 1)

    whole_b = jnp.sum(sb_pair[...], axis=0) + sb_keep[last]
    whole_a = jnp.sum(sa_all[...], axis=0) + sa_pair[...]
    mean_a = whole_a[0:1, :] * (1.0 / total_tokens)
    var_a = whole_a[1:2, :] * (1.0 / total_tokens) - mean_a * mean_a
    inv_a = 1.0 / jnp.sqrt(var_a + 1e-05)
    mean_b = whole_b[0:1, :] * (1.0 / total_tokens)
    var_b = whole_b[1:2, :] * (1.0 / total_tokens) - mean_b * mean_b
    inv_b = 1.0 / jnp.sqrt(var_b + 1e-05)
    for i in range(band // LANES):
        lanes = slice(i * LANES, (i + 1) * LANES)
        mean_col = column(mean_b[:, lanes])
        inv_col = column(inv_b[:, lanes])
        for c in range(own // LANES):
            cols = slice(c * LANES, (c + 1) * LANES)
            centered = held[last, lanes, cols] * (1.0 / total_tokens) - mean_col * mean_a[:, cols]
            out[lanes, cols] = centered * (inv_col * inv_a[:, cols])

    send_near_a.wait_send()

    @pl.loop(0, last)
    def _(p):
        send_far_a(p).wait_send()
        send_far_sums(p).wait_send()
        send_far(p).wait_send()

    @pl.loop(0, rings)
    def _(p):
        send_cross(p).wait_send()
        send_cross_sums(p).wait_send()

    @pl.loop(0, groups)
    def _(s):
        to_across(s).wait_send()
        to_partner(s).wait_send()
        forward(s).wait_send()


def fused(groups, act_a, act_b):
    tokens, own = act_a.shape
    rows, units = act_b.shape
    band = units // groups
    rings = groups // 2
    last = rings - 1
    dma = lambda n: pltpu.SemaphoreType.DMA((n,))
    return pl.pallas_call(
        functools.partial(kernel, groups, pair_order(rings)),
        out_shape=jax.ShapeDtypeStruct((band, own), jnp.float32),
        in_specs=[pl.BlockSpec(memory_space=pltpu.HBM)] * 2,
        out_specs=pl.BlockSpec(memory_space=pltpu.VMEM),
        scratch_shapes=[
            pltpu.VMEM((tokens, own), jnp.bfloat16),
            pltpu.VMEM((groups, tokens, band), jnp.bfloat16),
            pltpu.VMEM((rings, band, own), jnp.bfloat16),
            pltpu.VMEM((rings, band, own), jnp.bfloat16),
            pltpu.VMEM((last, band, own), jnp.bfloat16),
            pltpu.VMEM((last, band, own), jnp.bfloat16),
            pltpu.VMEM((rings, band, own), jnp.float32),
            pltpu.VMEM((8, own), jnp.float32),
            pltpu.VMEM((8, own), jnp.float32),
            pltpu.VMEM((8, own), jnp.float32),
            pltpu.VMEM((last, 8, own), jnp.float32),
            pltpu.VMEM((rings, 8, band), jnp.float32),
            pltpu.VMEM((rings, 8, band), jnp.float32),
            pltpu.VMEM((rings, 8, band), jnp.float32),
            pltpu.VMEM((last, 8, band), jnp.float32),
            pltpu.SemaphoreType.DMA,
            dma(groups),
            dma(groups), dma(groups),
            dma(groups), dma(groups),
            dma(groups), dma(groups),
            dma(rings), dma(rings),
            dma(last), dma(last),
            dma(rings), dma(rings),
            dma(last), dma(last),
            dma(1), dma(1),
            dma(last), dma(last),
        ],
        compiler_params=pltpu.CompilerParams(
            collective_id=0, has_side_effects=True, vmem_limit_bytes=60000 * 1024
        ),
        name="gather_correlate",
    )(act_a, act_b)


def solution(mesh):
    groups, split = mesh.shape["tok"], mesh.shape["unit"]

    def per_device(act_a, act_b):
        band = act_b.shape[1] // groups
        whole = act_a.shape[0] % 128 == 0 and act_a.shape[1] % LANES == 0
        if split == 4 and groups % 2 == 0 and groups > 4 and band % LANES == 0 and whole:
            return fused(groups, act_a, act_b)
        return plain(act_a, act_b)

    placed = (P("tok", "unit"), P(("tok", "unit"), None))
    return jax.shard_map(
        per_device, mesh=mesh, in_specs=placed, out_specs=P("tok", "unit"), check_vma=False
    )
```
